128 devices in a mesh: lat: 8 (over y, core), lon: 4 (over x), lev: 4 (over z).
Axes of the slice: x: 4, y: 4, z: 4, core: 2. Of those that a mesh axis runs over, the one named last changes fastest.
Arguments:
- tracer: float32 [32, 512, 128, 128], P('lat', 'lon', 'lev'), may hold values from 0.5 to 2
- conductance: float32 [32, 512, 128, 128], P('lat', 'lon', 'lev'), may hold values from 0.03 to 0.15
- source: float32 [32, 512, 128, 128], P('lat', 'lon', 'lev'), may hold values from -0.2 to 0.2
Outputs:
- standardized: float32 [32, 512, 128, 128], P('lat', 'lon', 'lev')
- tracer_end: float32 [32, 512, 128, 128], P('lat', 'lon', 'lev')
The draws below stay inside these ranges and needn't reach their ends.
All inputs are finite; a program needn't handle non-finite values.
Results may differ from the reference program's by a relative error of at most 0.00002.
Values sent between devices are 32-bit elements; how exact they have to be, the bound alone decides.
No kernel may reach another device: no remote copies, remote signals or barrier semaphores. Data moves between devices by JAX's collectives and lax.ppermute only.
A program may use at most 128 MiB of HBM per device.

```python
import jax
import jax.numpy as jnp
from jax import lax

GRID_J = 32
GRID_I = 512
GRID_K = 128
MEMBERS = 128
STEPS = 3


def shard_levels(stream_key, extent, cuts, smallest, top_value):
    def one(dim, shards_of):
        draws = jax.random.uniform(jax.random.fold_in(jax.random.fold_in(stream_key, 6), dim), (shards_of,), jnp.float32, smallest / len(cuts), top_value / len(cuts))
        return jnp.repeat(jnp.exp(draws), extent[dim] // shards_of).reshape((-1,) + (1,) * (len(extent) - dim - 1))

    level = one(*cuts[0])
    for cut in cuts[1:]:
        level = level * one(*cut)
    return level


def setup_inputs(seed: int = 0) -> dict:
    seeds = jax.random.split(jax.random.key(seed), 4)
    return {
        "tracer": jnp.clip(0.5 + 1.5 * jax.random.uniform(seeds[0], (GRID_J, GRID_I, GRID_K, MEMBERS), jnp.float32) ** shard_levels(seeds[0], (GRID_J, GRID_I, GRID_K, MEMBERS), ((0, 8), (1, 4), (2, 4)), -0.2, 0.2), 0.5, 2.0),
        "conductance": jnp.clip(0.03 + 0.120000007 * jax.random.uniform(seeds[1], (GRID_J, GRID_I, GRID_K, MEMBERS), jnp.float32) ** shard_levels(seeds[1], (GRID_J, GRID_I, GRID_K, MEMBERS), ((0, 8), (1, 4), (2, 4)), -0.2, 0.2), 0.03, 0.15),
        "source": jnp.clip(jax.random.uniform(seeds[2], (GRID_J, GRID_I, GRID_K, MEMBERS), jnp.float32, -0.2, 0.2) * shard_levels(seeds[2], (GRID_J, GRID_I, GRID_K, MEMBERS), ((0, 8), (1, 4), (2, 4)), -0.4, 0.0), -0.2, 0.2),
    }


def inner_cells(values, dims):
    for dim in dims:
        values = lax.slice_in_dim(values, 1, values.shape[dim] - 1, axis=dim)
    return values

def side_cells(values, dim, start, dims):
    others = [other for other in dims if other != dim]
    values = inner_cells(values, others)
    return lax.slice_in_dim(values, start, start + values.shape[dim] - 2, axis=dim)

def advance(padded, conductance, source):
    middle = inner_cells(padded, (0, 1, 2))
    lower = [side_cells(padded, dim, 0, (0, 1, 2)) for dim in (0, 1, 2)]
    upper = [side_cells(padded, dim, 2, (0, 1, 2)) for dim in (0, 1, 2)]
    spread = lower[0] + upper[0] + lower[1] + upper[1] + lower[2] + upper[2] - 6.0 * middle
    return middle + conductance * spread + source

def reference(tracer, conductance, source):
    for step in range(STEPS):
        tracer = advance(jnp.pad(tracer, ((1, 1), (1, 1), (1, 1), (0, 0)), mode='constant'), conductance, source)
    line_mean = lax.optimization_barrier(jnp.mean(tracer, axis=1, keepdims=True))
    centred = tracer - line_mean
    line_variance = lax.optimization_barrier(jnp.mean(centred * centred, axis=1, keepdims=True))
    standardized = centred * lax.rsqrt(line_variance + 0.0001)
    return (standardized, tracer)
```

```python
import jax
import jax.numpy as jnp
from jax import lax
from jax.experimental import pallas as pl
from jax.experimental.pallas import tpu as pltpu
from jax.sharding import PartitionSpec as P

STEPS = 3
F32 = jnp.float32
VMEM = pltpu.MemorySpace.VMEM
HBM = pltpu.MemorySpace.HBM
NJ, NI, NK, NM = 4, 128, 32, 128
PLANE = (NI, NK, NM)
UNROLL = 8


def call(kernel, name, args, outs, scratch=(), aliases=None, limit=4 << 20):
    arrays, in_specs = [], []
    for array, space in args:
        in_specs.append(pl.BlockSpec(memory_space=pl.ANY if space is HBM else space))
        arrays.append(pltpu.with_memory_space_constraint(array, space))
    return pl.pallas_call(
        kernel,
        out_shape=tuple(space(shape, F32) for shape, space in outs),
        in_specs=in_specs,
        out_specs=tuple(pl.BlockSpec(memory_space=pl.ANY if space is HBM else space) for _, space in outs),
        scratch_shapes=list(scratch),
        input_output_aliases=aliases or {},
        compiler_params=pltpu.CompilerParams(vmem_limit_bytes=limit),
        name=name,
    )(*arrays)


def row_of(p):
    odd = lax.rem(lax.axis_index("lat"), 2)
    return odd * p + (1 - odd) * (NJ - 1 - p)


def messages(tracer, cross, on, lon_low, lon_high, lev_low, lev_high, sems):
    copies = []

    def copy(src, dst):
        c = pltpu.make_async_copy(src, dst, sems.at[len(copies)])
        c.start()
        copies.append(c)

    copy(tracer.at[row_of(NJ - 1)], cross)
    copy(tracer.at[row_of(0)], on)
    for p in range(NJ):
        j = row_of(p)
        copy(tracer.at[j, 0], lon_low.at[p])
        copy(tracer.at[j, NI - 1], lon_high.at[p])
        copy(tracer.at[j, :, 0, :], lev_low.at[p])
        copy(tracer.at[j, :, NK - 1, :], lev_high.at[p])
    for c in copies:
        c.wait()


def advance(x, below, above, lon_low, lon_high, lev_low, lev_high, c, s, out, lev_outs=None, stats=None):
    def block(b, carry):
        i0 = pl.multiple_of(b * UNROLL, UNROLL)
        low, high = (lev_low[pl.ds(i0, UNROLL), :], lev_high[pl.ds(i0, UNROLL), :])
        before = jnp.where(b == 0, lon_low[...], x[jnp.maximum(i0 - 1, 0)])
        here = x[i0]
        for r in range(UNROLL):
            if r < UNROLL - 1:
                after = x[i0 + r + 1]
            else:
                after = jnp.where(b == NI // UNROLL - 1, lon_high[...], x[jnp.minimum(i0 + UNROLL, NI - 1)])
            down = jnp.concatenate([low[r : r + 1], here[: NK - 1]], axis=0)
            up = jnp.concatenate([here[1:], high[r : r + 1]], axis=0)
            spread = (before + after) + (below[i0 + r] + above[i0 + r]) + (down + up) - 6.0 * here
            new = here + c[i0 + r] * spread + s[i0 + r]
            out[i0 + r] = new
            if lev_outs is not None:
                lev_outs[0][pl.ds(i0 + r, 1), :] = new[0:1]
                lev_outs[1][pl.ds(i0 + r, 1), :] = new[NK - 1 : NK]
            if stats is not None:
                shift, total, squares = carry
                if r == 0:
                    shift = jnp.where(b == 0, new, shift)
                moved = new - shift
                carry = (shift, total + moved, squares + moved * moved)
            before, here = here, after
        return carry

    zero = jnp.zeros((NK, NM), F32)
    carry = lax.fori_loop(0, NI // UNROLL, block, (zero, zero, zero) if stats is not None else 0)
    if stats is not None:
        shift, total, squares = carry
        stats[0][...] = shift + total * (1.0 / NI)
        stats[1][...] = squares - total * (total * (1.0 / NI))


def interior_first(tracer, c, s, on, lon_low, lon_high, lev_low, lev_high, q0, q1, q2, lonl, lonh, levl, levh):
    outs = (q0, q1, q2)
    for p in range(3):
        j = row_of(p)
        below = on if p == 0 else tracer.at[row_of(p - 1)]
        advance(
            tracer.at[j], below, tracer.at[row_of(p + 1)], lon_low.at[p], lon_high.at[p], lev_low.at[p], lev_high.at[p],
            c.at[j], s.at[j], outs[p], (levl.at[p], levh.at[p]),
        )
        lonl[p] = outs[p][0]
        lonh[p] = outs[p][NI - 1]


def boundary_first(tracer, c, s, cross, lon_low, lon_high, lev_low, lev_high, a0, a1, a2, a3, q3, lonl, lonh, levl, levh):
    p = 3
    j = row_of(p)
    advance(
        tracer.at[j], tracer.at[row_of(p - 1)], cross, lon_low.at[p], lon_high.at[p], lev_low.at[p], lev_high.at[p],
        c.at[j], s.at[j], q3, (levl.at[p], levh.at[p]),
    )
    lonl[p] = q3[0]
    lonh[p] = q3[NI - 1]


def interior(x0, x1, x2, x3, c, s, on, lon_low, lon_high, lev_low, lev_high, q0, q1, q2, lonl, lonh, levl, levh):
    xs, outs = ((x0, x1, x2, x3), (q0, q1, q2))
    for p in range(3):
        j = row_of(p)
        advance(
            xs[p], on if p == 0 else xs[p - 1], xs[p + 1], lon_low.at[p], lon_high.at[p], lev_low.at[p], lev_high.at[p],
            c.at[j], s.at[j], outs[p], (levl.at[p], levh.at[p]),
        )
        lonl[p] = outs[p][0]
        lonh[p] = outs[p][NI - 1]


def boundary(x2, x3, c, s, cross, lon_low, lon_high, lev_low, lev_high, a0, a1, a2, a3, q3, lonl, lonh, levl, levh):
    p = 3
    j = row_of(p)
    advance(
        x3, x2, cross, lon_low.at[p], lon_high.at[p], lev_low.at[p], lev_high.at[p],
        c.at[j], s.at[j], q3, (levl.at[p], levh.at[p]),
    )
    lonl[p] = q3[0]
    lonh[p] = q3[NI - 1]


def interior_last(x0, x1, x2, x3, c, s, on, lon_low, lon_high, lev_low, lev_high, q0, q1, q2, stats, end, sems):
    xs, outs = ((x0, x1, x2, x3), (q0, q1, q2))
    copies = []
    for p in range(3):
        j = row_of(p)
        advance(
            xs[p], on if p == 0 else xs[p - 1], xs[p + 1], lon_low.at[p], lon_high.at[p], lev_low.at[p], lev_high.at[p],
            c.at[j], s.at[j], outs[p], None, (stats.at[0, p], stats.at[1, p]),
        )
        copies.append(pltpu.make_async_copy(outs[p], end.at[j], sems.at[p]))
        copies[-1].start()
    for copy in copies:
        copy.wait()


def boundary_last(x2, x3, c, s, cross, lon_low, lon_high, lev_low, lev_high, a0, a1, q3, stats, end, sem):
    p = 3
    j = row_of(p)
    advance(
        x3, x2, cross, lon_low.at[p], lon_high.at[p], lev_low.at[p], lev_high.at[p],
        c.at[j], s.at[j], q3, None, (stats.at[0, p], stats.at[1, p]),
    )
    copy = pltpu.make_async_copy(q3, end.at[j], sem)
    copy.start()
    copy.wait()


def scaled(parts):
    def kernel(q0, q1, q2, q3, stats, out, buffers, sems):
        copies = []
        for p, q in enumerate((q0, q1, q2, q3)):
            means = [stats[d, 0, p] for d in range(parts)]
            mean = sum(means[1:], means[0]) * (1.0 / parts)
            square = sum([stats[d, 1, p] for d in range(1, parts)], stats[0, 1, p])
            for m in means:
                square = square + NI * ((m - mean) * (m - mean))
            scale = lax.rsqrt(square * (1.0 / (parts * NI)) + 0.0001)
            slot = p % 2
            if p >= 2:
                copies[p - 2].wait()

            def block(b, _):
                i0 = b * UNROLL
                for r in range(UNROLL):
                    buffers[slot, i0 + r] = (q[i0 + r] - mean) * scale
                return 0

            lax.fori_loop(0, NI // UNROLL, block, 0)
            copies.append(pltpu.make_async_copy(buffers.at[slot], out.at[row_of(p)], sems.at[p]))
            copies[-1].start()
        for copy in copies[2:]:
            copy.wait()

    return kernel


def shards(tracer, c, s):
    lats, lons, levs = (lax.axis_size(a) for a in ("lat", "lon", "lev"))
    on_pairs = [(i, i ^ 1) for i in range(lats)]
    cross_pairs = [(i, ((i + 1) ^ 1) - 1) for i in range(lats) if 0 <= ((i + 1) ^ 1) - 1 < lats]

    def to_next(array, axis):
        n = lax.axis_size(axis)
        return lax.ppermute(array, axis, [(i, i + 1) for i in range(n - 1)])

    def to_previous(array, axis):
        n = lax.axis_size(axis)
        return lax.ppermute(array, axis, [(i + 1, i) for i in range(n - 1)])

    def faces(lonl, lonh, levl, levh):
        lev = (to_next(levh, "lev"), to_previous(levl, "lev"))
        lon = (to_next(lonh, "lon"), to_previous(lonl, "lon"))
        return [(a, VMEM) for a in (*lon, *lev)]

    lon_face, lev_face = ((NJ, NK, NM), (NJ, NI, NM))
    face_outs = [(lon_face, VMEM)] * 2 + [(lev_face, VMEM)] * 2
    planes = lambda n: [(PLANE, VMEM)] * n
    dma = pltpu.SemaphoreType.DMA

    msg = call(
        messages, "messages", [(tracer, HBM)], planes(2) + face_outs, scratch=[dma((2 + 4 * NJ,))]
    )
    cross = lax.ppermute(msg[0], "lat", cross_pairs)
    on = lax.ppermute(msg[1], "lat", on_pairs)
    halo = faces(*msg[2:])
    cs = [(c, VMEM), (s, VMEM)]

    x = None
    for step in range(STEPS):
        last = step == STEPS - 1
        now = [(tracer, VMEM)] if step == 0 else [(q, VMEM) for q in x]
        pair = now if step == 0 else now[2:]
        if last:
            q0, q1, q2, stats, end = call(
                interior_last, "interior_last", now + cs + [(on, VMEM)] + halo,
                planes(3) + [((2, NJ, NK, NM), VMEM), ((NJ, *PLANE), HBM)], scratch=[dma((3,))],
            )
            n = len(pair) + 7
            q3, stats, end = call(
                boundary_last, "boundary_last", pair + cs + [(cross, VMEM)] + halo + [(stats, VMEM), (end, HBM)],
                planes(1) + [((2, NJ, NK, NM), VMEM), ((NJ, *PLANE), HBM)], scratch=[dma(())],
                aliases={n: 1, n + 1: 2},
            )
        else:
            q0, q1, q2, *out_faces = call(
                interior if step else interior_first, f"interior{step}", now + cs + [(on, VMEM)] + halo, planes(3) + face_outs,
            )
            n = len(pair) + 7
            on = lax.ppermute(q0, "lat", on_pairs)
            q3, *out_faces = call(
                boundary if step else boundary_first, f"boundary{step}",
                pair + cs + [(cross, VMEM)] + halo + [(f, VMEM) for f in out_faces], planes(1) + face_outs,
                aliases={n + k: 1 + k for k in range(4)},
            )
            cross = lax.ppermute(q3, "lat", cross_pairs)
            halo = faces(*out_faces)
        x = (q0, q1, q2, q3)

    everyone = lax.all_gather(stats, "lon")
    (out,) = call(
        scaled(lons), "scaled", [(q, VMEM) for q in x] + [(everyone, VMEM)], [((NJ, *PLANE), HBM)],
        scratch=[pltpu.VMEM((2, *PLANE), F32), dma((NJ,))], limit=8 << 20,
    )
    return out, end


def solution(mesh):
    placed = P("lat", "lon", "lev", None)
    return jax.shard_map(
        shards, mesh=mesh, in_specs=(placed, placed, placed), out_specs=(placed, placed), check_vma=False
    )
```

```python
import jax
import jax.numpy as jnp
from jax import lax
from jax.experimental import pallas as pl
from jax.experimental.pallas import tpu as pltpu
from jax.sharding import PartitionSpec as P


STEPS = 3
F32 = jnp.float32
VMEM = pltpu.MemorySpace.VMEM
HBM = pltpu.MemorySpace.HBM
NJ, NI, NK, NM = 4, 128, 32, 128
HALF = NI // 2
PLANE = (NI, NK, NM)
HALF_PLANE = (HALF, NK, NM)
FACES = ((NJ, NK, NM),) * 2 + ((NJ, NI, NM),) * 2
UNROLL = 8


def call(kernel, args, outs, scratch=(), aliases=None, limit=4 << 20):
    arrays, in_specs = [], []
    for array, space in args:
        in_specs.append(pl.BlockSpec(memory_space=pl.ANY if space is HBM else space))
        arrays.append(pltpu.with_memory_space_constraint(array, space))
    return pl.pallas_call(
        kernel,
        out_shape=tuple(space(shape, F32) for shape, space in outs),
        in_specs=in_specs,
        out_specs=tuple(pl.BlockSpec(memory_space=pl.ANY if space is HBM else space) for _, space in outs),
        scratch_shapes=list(scratch),
        input_output_aliases=aliases or {},
        compiler_params=pltpu.CompilerParams(vmem_limit_bytes=limit),
    )(*arrays)


def row_of(p):
    odd = lax.rem(lax.axis_index("lat"), 2)
    return odd * p + (1 - odd) * (NJ - 1 - p)


def start(src, dst, sem):
    copy = pltpu.make_async_copy(src, dst, sem)
    copy.start()
    return copy


def messages(tracer, x3a, x3b, x0, lon_low, lon_high, lev_low, lev_high, sems):
    pairs = [
        (tracer.at[row_of(3), pl.ds(0, HALF)], x3a),
        (tracer.at[row_of(3), pl.ds(HALF, HALF)], x3b),
        (tracer.at[row_of(0)], x0),
    ]
    for p in range(NJ):
        j = row_of(p)
        pairs += [
            (tracer.at[j, :, 0, :], lev_low.at[p]),
            (tracer.at[j, :, NK - 1, :], lev_high.at[p]),
            (tracer.at[j, 0], lon_low.at[p]),
            (tracer.at[j, NI - 1], lon_high.at[p]),
        ]
    copies = [start(src, dst, sems.at[n]) for n, (src, dst) in enumerate(pairs)]
    for copy in copies:
        copy.wait()


def load_edge(tracer, c, s, x2, c3, s3, sems):
    pairs = [(tracer.at[row_of(2)], x2), (c.at[row_of(3)], c3), (s.at[row_of(3)], s3)]
    copies = [start(src, dst, sems.at[n]) for n, (src, dst) in enumerate(pairs)]
    for copy in copies:
        copy.wait()


def advance(x, before, after, below, above, lev_low, lev_high, c, s, out, lev_outs=None, sums=None):
    def at(view, i, size=None):
        ref, first = view
        return ref[first + i] if size is None else ref[pl.ds(pl.multiple_of(first + i, UNROLL), size), :]

    def block(b, carry):
        i0 = b * UNROLL
        low, high = (at(lev_low, i0, UNROLL), at(lev_high, i0, UNROLL))
        prev = jnp.where(b == 0, before, at(x, jnp.maximum(i0 - 1, 0)))
        here = at(x, i0)
        for r in range(UNROLL):
            if r < UNROLL - 1:
                nxt = at(x, i0 + r + 1)
            else:
                nxt = jnp.where(b == HALF // UNROLL - 1, after, at(x, jnp.minimum(i0 + UNROLL, HALF - 1)))
            down = jnp.concatenate([low[r : r + 1], here[: NK - 1]], axis=0)
            up = jnp.concatenate([here[1:], high[r : r + 1]], axis=0)
            spread = (prev + nxt) + (at(below, i0 + r) + at(above, i0 + r)) + (down + up) - 6.0 * here
            new = here + at(c, i0 + r) * spread + at(s, i0 + r)
            out[0][out[1] + i0 + r] = new
            if lev_outs is not None:
                for (ref, first), k in zip(lev_outs, (0, NK - 1)):
                    ref[pl.ds(first + i0 + r, 1), :] = new[k : k + 1]
            if sums is not None:
                shift, total, squares = carry
                if r == 0 and sums[0] is None:
                    shift = jnp.where(b == 0, new, shift)
                moved = new - shift
                carry = (shift, total + moved, squares + moved * moved)
            prev, here = here, nxt
        return carry

    if sums is None:
        first = 0
    else:
        first = (jnp.zeros((NK, NM), F32) if sums[0] is None else sums[0], *sums[1:])
    return lax.fori_loop(0, HALF // UNROLL, block, first)


def put_stats(stats, p, sums):
    shift, total, squares = sums
    mean, square = (shift + total * (1.0 / NI), squares - total * (total * (1.0 / NI)))
    for d in range(stats.shape[0]):
        stats[d, 0, p] = mean
        stats[d, 1, p] = square


def no_sums():
    zero = jnp.zeros((NK, NM), F32)
    return (None, zero, zero)


def inner_planes(xs, on, halo, cs, outs, faces=None, stats=None, ready=lambda p: None, done=lambda p: None):
    lon_low, lon_high, lev_low, lev_high = halo
    for p in (2, 1, 0):
        ready(p)
        x, out = xs[p], outs[p]
        sums = no_sums() if stats is not None else None
        for h in (0, 1):
            first = h * HALF
            below = (on, first) if p == 0 else (xs[p - 1], first)
            above = (xs[3 + h], 0) if p == 2 else (xs[p + 1], first)
            before = x[HALF - 1] if h else lon_low[p]
            after = lon_high[p] if h else x[HALF]
            sums = advance(
                (x, first), before, after, below, above, (lev_low.at[p], first), (lev_high.at[p], first),
                (cs[p][0], first), (cs[p][1], first), (out, first),
                None if faces is None else ((faces[2].at[p], first), (faces[3].at[p], first)),
                sums if stats is not None else None,
            )
        if faces is not None:
            faces[0][p] = out[0]
            faces[1][p] = out[NI - 1]
        if stats is not None:
            put_stats(stats, p, sums)
        done(p)


def edge_half(h, x2, x3, cross, halo, c3, s3, out, faces=None, sums=None):
    lon_low, lon_high, lev_low, lev_high = halo
    p, first = 3, h * HALF
    sums = advance(
        (x3[h], 0), x3[0][HALF - 1] if h else lon_low[p], lon_high[p] if h else x3[1][0],
        (x2, first), (cross, 0), (lev_low.at[p], first), (lev_high.at[p], first), (c3, first), (s3, first), (out, 0),
        None if faces is None else ((faces[2].at[p], first), (faces[3].at[p], first)), sums,
    )
    if faces is not None:
        if h:
            faces[1][p] = out[HALF - 1]
        else:
            faces[0][p] = out[0]
    return sums


def edge_a(x2, x3a, x3b, cross, ll, lh, vl, vh, c3, s3, out, *faces):
    edge_half(0, x2, (x3a, x3b), cross, (ll, lh, vl, vh), c3, s3, out, faces)


def edge_b(x2, x3a, x3b, cross, ll, lh, vl, vh, c3, s3, a0, a1, a2, a3, out, *faces):
    edge_half(1, x2, (x3a, x3b), cross, (ll, lh, vl, vh), c3, s3, out, faces)


def edge_a_last(x2, x3a, x3b, cross, ll, lh, vl, vh, c3, s3, out, raw):
    sums = edge_half(0, x2, (x3a, x3b), cross, (ll, lh, vl, vh), c3, s3, out, None, no_sums())
    for n in range(3):
        raw[n] = sums[n]


def edge_b_last(x2, x3a, x3b, cross, ll, lh, vl, vh, c3, s3, raw, a0, out, stats):
    sums = (raw[0], raw[1], raw[2])
    put_stats(stats, 3, edge_half(1, x2, (x3a, x3b), cross, (ll, lh, vl, vh), c3, s3, out, None, sums))


def inner_first(
    tracer, c, s, x0, x2, x3a, x3b, on, ll, lh, vl, vh, a0, a1, a2, a3, q0, q1, q2, f0, f1, f2, f3, cc, ss, x1, sems
):
    loads = [[start(tracer.at[row_of(1)], x1, sems.at[6])], [], []]
    for p in (2, 1, 0):
        loads[p] += [start(c.at[row_of(p)], cc.at[p], sems.at[p]), start(s.at[row_of(p)], ss.at[p], sems.at[3 + p])]
    loads[2] += loads[0][:1]
    loads[0] = loads[0][1:]

    def ready(p):
        for copy in loads[p]:
            copy.wait()

    inner_planes(
        (x0, x1, x2, x3a, x3b), on, (ll, lh, vl, vh), [(cc.at[p], ss.at[p]) for p in range(3)], (q0, q1, q2),
        (f0, f1, f2, f3), ready=ready,
    )


def inner(x0, x1, x2, x3a, x3b, on, ll, lh, vl, vh, cc, ss, a0, a1, a2, a3, q0, q1, q2, *faces):
    inner_planes(
        (x0, x1, x2, x3a, x3b), on, (ll, lh, vl, vh), [(cc.at[p], ss.at[p]) for p in range(3)], (q0, q1, q2), faces
    )


def inner_last(x0, x1, x2, x3a, x3b, on, ll, lh, vl, vh, cc, ss, raw, q0, q1, q2, stats, end, sems):
    outs, copies = ((q0, q1, q2), [])
    inner_planes(
        (x0, x1, x2, x3a, x3b), on, (ll, lh, vl, vh), [(cc.at[p], ss.at[p]) for p in range(3)], outs, None, stats,
        done=lambda p: copies.append(start(outs[p], end.at[row_of(p)], sems.at[p])),
    )
    for copy in copies:
        copy.wait()


def scaled(q0, q1, q2, q3a, q3b, stats, a0, out, end, buffers, sems):
    parts = stats.shape[0]
    last = [start(q, end.at[row_of(3), pl.ds(h * HALF, HALF)], sems.at[NJ + h]) for h, q in enumerate((q3a, q3b))]
    copies = []
    for p in range(NJ):
        means = [stats[d, 0, p] for d in range(parts)]
        mean = sum(means[1:], means[0]) * (1.0 / parts)
        square = sum([stats[d, 1, p] for d in range(1, parts)], stats[0, 1, p])
        for m in means:
            square = square + NI * ((m - mean) * (m - mean))
        scale = lax.rsqrt(square * (1.0 / (parts * NI)) + 0.0001)
        slot = p % 2
        if p >= 2:
            copies[p - 2].wait()
        for first, q in ((0, (q0, q1, q2)[p]),) if p < 3 else ((0, q3a), (HALF, q3b)):

            def block(b, _, first=first, q=q):
                i0 = b * UNROLL
                for r in range(UNROLL):
                    buffers[slot, first + i0 + r] = (q[i0 + r] - mean) * scale
                return 0

            lax.fori_loop(0, q.shape[0] // UNROLL, block, 0)
        copies.append(start(buffers.at[slot], out.at[row_of(p)], sems.at[p]))
    for copy in (*copies[2:], *last):
        copy.wait()


def shards(tracer, c, s):
    lats, lons = (lax.axis_size(a) for a in ("lat", "lon"))
    on_pairs = [(i, i ^ 1) for i in range(lats)]
    cross_pairs = [(i, ((i + 1) ^ 1) - 1) for i in range(lats) if 0 <= ((i + 1) ^ 1) - 1 < lats]

    def to_next(array, axis):
        return lax.ppermute(array, axis, [(i, i + 1) for i in range(lax.axis_size(axis) - 1)])

    def to_previous(array, axis):
        return lax.ppermute(array, axis, [(i + 1, i) for i in range(lax.axis_size(axis) - 1)])

    def exchanged(faces):
        lon_low, lon_high, lev_low, lev_high = faces
        lev = (to_next(lev_high, "lev"), to_previous(lev_low, "lev"))
        return [to_next(lon_high, "lon"), to_previous(lon_low, "lon"), *lev]

    def swapped(q, pairs):
        return lax.ppermute(q, "lat", pairs)

    vm = lambda *arrays: [(a, VMEM) for a in arrays]
    dma = pltpu.SemaphoreType.DMA
    half, plane, face_outs = ((HALF_PLANE, VMEM), (PLANE, VMEM), [(f, VMEM) for f in FACES])
    inner_fields = ((3, *PLANE), VMEM)

    x3a, x3b, x0, *faces = call(
        messages, [(tracer, HBM)], [half, half, plane] + face_outs, scratch=[dma((3 + 4 * NJ,))]
    )
    cross = [swapped(x3a, cross_pairs), swapped(x3b, cross_pairs)]
    on = swapped(x0, on_pairs)
    halo = exchanged(faces)
    x2, c3, s3 = call(load_edge, [(a, HBM) for a in (tracer, c, s)], [plane] * 3, scratch=[dma((3,))])

    for step in range(STEPS):
        edge = vm(x2, x3a, x3b)
        rest = vm(*halo, c3, s3)
        if step < STEPS - 1:
            qa, *faces = call(edge_a, edge + vm(cross[0]) + rest, [half] + face_outs)
            cross[0] = swapped(qa, cross_pairs)
            outs = [plane] * 3 + face_outs
            if step == 0:
                q0, q1, q2, *faces, cc, ss = call(
                    inner_first,
                    [(a, HBM) for a in (tracer, c, s)] + vm(x0, x2, x3a, x3b, on, *halo, *faces),
                    outs + [inner_fields] * 2, scratch=[pltpu.VMEM(PLANE, F32), dma((7,))],
                    aliases={12 + n: 3 + n for n in range(4)}, limit=6 << 20,
                )
            else:
                q0, q1, q2, *faces = call(
                    inner, vm(x0, x1, x2, x3a, x3b, on, *halo, cc, ss, *faces), outs,
                    aliases={12 + n: 3 + n for n in range(4)},
                )
            on = swapped(q0, on_pairs)
            qb, *faces = call(
                edge_b, edge + vm(cross[1]) + rest + vm(*faces), [half] + face_outs,
                aliases={10 + n: 1 + n for n in range(4)},
            )
            cross[1] = swapped(qb, cross_pairs)
            halo = exchanged(faces)
        else:
            qa, raw = call(edge_a_last, edge + vm(cross[0]) + rest, [half, ((3, NK, NM), VMEM)])
            all_stats = ((lons, 2, NJ, NK, NM), VMEM)
            q0, q1, q2, stats, end = call(
                inner_last, vm(x0, x1, x2, x3a, x3b, on, *halo, cc, ss, raw),
                [plane] * 3 + [all_stats, ((NJ, *PLANE), HBM)], scratch=[dma((3,))],
            )
            qb, stats = call(
                edge_b_last, edge + vm(cross[1]) + rest + vm(raw, stats), [half, all_stats],
                aliases={11: 1},
            )
        x0, x1, x2, x3a, x3b = q0, q1, q2, qa, qb

    everyone = lax.all_to_all(stats, "lon", 0, 0, tiled=True)
    out, end = call(
        scaled, vm(x0, x1, x2, x3a, x3b, everyone) + [(end, HBM)], [((NJ, *PLANE), HBM)] * 2,
        scratch=[pltpu.VMEM((2, *PLANE), F32), dma((NJ + 2,))], aliases={6: 1}, limit=8 << 20,
    )
    return out, end


def solution(mesh):
    placed = P("lat", "lon", "lev", None)

    return jax.shard_map(
        shards, mesh=mesh, in_specs=(placed, placed, placed), out_specs=(placed, placed), check_vma=False
    )
```

```python
import jax
import jax.numpy as jnp
from jax import lax
from jax.experimental import pallas as pl
from jax.experimental.pallas import tpu as pltpu
from jax.sharding import PartitionSpec as P


STEPS = 3
F32 = jnp.float32
VMEM = pltpu.MemorySpace.VMEM
HBM = pltpu.MemorySpace.HBM
NJ, NI, NK, NM = 4, 128, 32, 128
HALF = NI // 2
PLANE = (NI, NK, NM)
HALF_PLANE = (HALF, NK, NM)
FACES = ((NJ, NK, NM),) * 2 + ((NJ, NI, NM),) * 2
UNROLL = 8


def call(kernel, args, outs, scratch=(), aliases=None, limit=4 << 20):
    arrays, in_specs = [], []
    for array, space in args:
        in_specs.append(pl.BlockSpec(memory_space=pl.ANY if space is HBM else space))
        arrays.append(pltpu.with_memory_space_constraint(array, space))
    return pl.pallas_call(
        kernel,
        out_shape=tuple(space(shape, F32) for shape, space in outs),
        in_specs=in_specs,
        out_specs=tuple(pl.BlockSpec(memory_space=pl.ANY if space is HBM else space) for _, space in outs),
        scratch_shapes=list(scratch),
        input_output_aliases=aliases or {},
        compiler_params=pltpu.CompilerParams(vmem_limit_bytes=limit),
    )(*arrays)


def row_of(p):
    odd = lax.rem(lax.axis_index("lat"), 2)
    return odd * p + (1 - odd) * (NJ - 1 - p)


def at_end(axis, high):
    return lax.axis_index(axis) == (lax.axis_size(axis) - 1 if high else 0)


def unless(outside, values):
    return jnp.where(outside, jnp.zeros_like(values), values)


def start(src, dst, sem):
    copy = pltpu.make_async_copy(src, dst, sem)
    copy.start()
    return copy


def first(tracer, x3a, sem):
    start(tracer.at[row_of(3), pl.ds(0, HALF)], x3a, sem).wait()


def messages(tracer, x3b, x0, lon_low, lon_high, lev_low, lev_high, sems):
    pairs = [
        (tracer.at[row_of(3), pl.ds(HALF, HALF)], x3b),
        (tracer.at[row_of(0)], x0),
    ]
    for p in range(NJ):
        j = row_of(p)
        pairs += [
            (tracer.at[j, :, 0, :], lev_low.at[p]),
            (tracer.at[j, :, NK - 1, :], lev_high.at[p]),
            (tracer.at[j, 0], lon_low.at[p]),
            (tracer.at[j, NI - 1], lon_high.at[p]),
        ]
    copies = [start(src, dst, sems.at[n]) for n, (src, dst) in enumerate(pairs)]
    for copy in copies:
        copy.wait()


def load_edge(tracer, c, s, x2, c3, s3, sems):
    pairs = [(tracer.at[row_of(2)], x2), (c.at[row_of(3)], c3), (s.at[row_of(3)], s3)]
    copies = [start(src, dst, sems.at[n]) for n, (src, dst) in enumerate(pairs)]
    for copy in copies:
        copy.wait()


def advance(x, before, after, below, above, lev_low, lev_high, c, s, out, lev_outs=None, sums=None, top=False):
    def at(view, i, size=None):
        ref, first = view
        return ref[first + i] if size is None else ref[pl.ds(pl.multiple_of(first + i, UNROLL), size), :]

    def block(b, carry):
        i0 = b * UNROLL
        low = unless(at_end("lev", False), at(lev_low, i0, UNROLL))
        high = unless(at_end("lev", True), at(lev_high, i0, UNROLL))
        prev = jnp.where(b == 0, before, at(x, jnp.maximum(i0 - 1, 0)))
        here = at(x, i0)
        for r in range(UNROLL):
            if r < UNROLL - 1:
                nxt = at(x, i0 + r + 1)
            else:
                nxt = jnp.where(b == HALF // UNROLL - 1, after, at(x, jnp.minimum(i0 + UNROLL, HALF - 1)))
            down = jnp.concatenate([low[r : r + 1], here[: NK - 1]], axis=0)
            up = jnp.concatenate([here[1:], high[r : r + 1]], axis=0)
            over = at(above, i0 + r) if top is False else unless(top, at(above, i0 + r))
            spread = (prev + nxt) + (at(below, i0 + r) + over) + (down + up) - 6.0 * here
            new = here + at(c, i0 + r) * spread + at(s, i0 + r)
            out[0][out[1] + i0 + r] = new
            if lev_outs is not None:
                for (ref, first), k in zip(lev_outs, (0, NK - 1)):
                    ref[pl.ds(first + i0 + r, 1), :] = new[k : k + 1]
            if sums is not None:
                shift, total, squares = carry
                if r == 0 and sums[0] is None:
                    shift = jnp.where(b == 0, new, shift)
                moved = new - shift
                carry = (shift, total + moved, squares + moved * moved)
            prev, here = here, nxt
        return carry

    if sums is None:
        first = 0
    else:
        first = (jnp.zeros((NK, NM), F32) if sums[0] is None else sums[0], *sums[1:])
    return lax.fori_loop(0, HALF // UNROLL, block, first)


def put_stats(stats, p, sums):
    shift, total, squares = sums
    stats[0, p] = shift + total * (1.0 / NI)
    stats[1, p] = squares - total * (total * (1.0 / NI))


def no_sums():
    zero = jnp.zeros((NK, NM), F32)
    return (None, zero, zero)


def inner_planes(xs, on, halo, cs, outs, faces=None, stats=None, ready=lambda p: None, done=lambda p: None):
    lon_low, lon_high, lev_low, lev_high = halo
    for p in (2, 1, 0):
        ready(p)
        x, out = xs[p], outs[p]
        sums = no_sums() if stats is not None else None
        for h in (0, 1):
            first = h * HALF
            below = (on, first) if p == 0 else (xs[p - 1], first)
            above = (xs[3 + h], 0) if p == 2 else (xs[p + 1], first)
            before = x[HALF - 1] if h else unless(at_end("lon", False), lon_low[p])
            after = unless(at_end("lon", True), lon_high[p]) if h else x[HALF]
            sums = advance(
                (x, first), before, after, below, above, (lev_low.at[p], first), (lev_high.at[p], first),
                (cs[p][0], first), (cs[p][1], first), (out, first),
                None if faces is None else ((faces[2].at[p], first), (faces[3].at[p], first)),
                sums if stats is not None else None,
            )
        if faces is not None:
            faces[0][p] = out[0]
            faces[1][p] = out[NI - 1]
        if stats is not None:
            put_stats(stats, p, sums)
        done(p)


def edge_half(h, x2, x3, cross, halo, c3, s3, out, faces=None, sums=None):
    lon_low, lon_high, lev_low, lev_high = halo
    p, first = 3, h * HALF
    before = x3[0][HALF - 1] if h else unless(at_end("lon", False), lon_low[p])
    after = unless(at_end("lon", True), lon_high[p]) if h else x3[1][0]
    sums = advance(
        (x3[h], 0), before, after,
        (x2, first), (cross, 0), (lev_low.at[p], first), (lev_high.at[p], first), (c3, first), (s3, first), (out, 0),
        None if faces is None else ((faces[2].at[p], first), (faces[3].at[p], first)), sums,
        jnp.logical_or(at_end("lat", False), at_end("lat", True)),
    )
    if faces is not None:
        if h:
            faces[1][p] = out[HALF - 1]
        else:
            faces[0][p] = out[0]
    return sums


def edge_a(x2, x3a, x3b, cross, ll, lh, vl, vh, c3, s3, out, *faces):
    edge_half(0, x2, (x3a, x3b), cross, (ll, lh, vl, vh), c3, s3, out, faces)


def edge_b(x2, x3a, x3b, cross, ll, lh, vl, vh, c3, s3, a0, a1, a2, a3, out, *faces):
    edge_half(1, x2, (x3a, x3b), cross, (ll, lh, vl, vh), c3, s3, out, faces)


def edge_a_last(x2, x3a, x3b, cross, ll, lh, vl, vh, c3, s3, out, raw):
    sums = edge_half(0, x2, (x3a, x3b), cross, (ll, lh, vl, vh), c3, s3, out, None, no_sums())
    for n in range(3):
        raw[n] = sums[n]


def edge_b_last(x2, x3a, x3b, cross, ll, lh, vl, vh, c3, s3, raw, out, stats):
    sums = (raw[0], raw[1], raw[2])
    put_stats(stats, 0, edge_half(1, x2, (x3a, x3b), cross, (ll, lh, vl, vh), c3, s3, out, None, sums))


def inner_first(
    tracer, c, s, x0, x2, x3a, x3b, on, ll, lh, vl, vh, a0, a1, a2, a3, q0, q1, q2, f0, f1, f2, f3, cc, ss, x1, sems
):
    loads = [[start(tracer.at[row_of(1)], x1, sems.at[6])], [], []]
    for p in (2, 1, 0):
        loads[p] += [start(c.at[row_of(p)], cc.at[p], sems.at[p]), start(s.at[row_of(p)], ss.at[p], sems.at[3 + p])]
    loads[2] += loads[0][:1]
    loads[0] = loads[0][1:]

    def ready(p):
        for copy in loads[p]:
            copy.wait()

    inner_planes(
        (x0, x1, x2, x3a, x3b), on, (ll, lh, vl, vh), [(cc.at[p], ss.at[p]) for p in range(3)], (q0, q1, q2),
        (f0, f1, f2, f3), ready=ready,
    )


def inner(x0, x1, x2, x3a, x3b, on, ll, lh, vl, vh, cc, ss, a0, a1, a2, a3, q0, q1, q2, *faces):
    inner_planes(
        (x0, x1, x2, x3a, x3b), on, (ll, lh, vl, vh), [(cc.at[p], ss.at[p]) for p in range(3)], (q0, q1, q2), faces
    )


def inner_last(x0, x1, x2, x3a, x3b, on, ll, lh, vl, vh, cc, ss, raw, q0, q1, q2, stats, end, sems):
    outs, copies = ((q0, q1, q2), [])
    inner_planes(
        (x0, x1, x2, x3a, x3b), on, (ll, lh, vl, vh), [(cc.at[p], ss.at[p]) for p in range(3)], outs, None, stats,
        done=lambda p: copies.append(start(outs[p], end.at[row_of(p)], sems.at[p])),
    )
    for copy in copies:
        copy.wait()


def scaled(parts, p, stats):
    means = [part[0, p] for part in stats]
    mean = sum(means[1:], means[0]) * (1.0 / parts)
    square = sum([part[1, p] for part in stats[1:]], stats[0][1, p])
    for m in means:
        square = square + NI * ((m - mean) * (m - mean))
    return mean, lax.rsqrt(square * (1.0 / (parts * NI)) + 0.0001)


def scale_rows(q, mean, scale, out):
    def block(b, _):
        i0 = b * UNROLL
        for r in range(UNROLL):
            out[i0 + r] = (q[i0 + r] - mean) * scale
        return 0

    lax.fori_loop(0, q.shape[0] // UNROLL, block, 0)


def scale_inner(parts):
    def kernel(q0, q1, q2, q3a, q3b, *rest):
        stats, (_, out, end, buffers, sems) = rest[:parts], rest[parts:]
        copies = [start(q, end.at[row_of(3), pl.ds(h * HALF, HALF)], sems.at[3 + h]) for h, q in enumerate((q3a, q3b))]
        for p, q in enumerate((q0, q1, q2)):
            scale_rows(q, *scaled(parts, p, stats), buffers.at[p])
            copies.append(start(buffers.at[p], out.at[row_of(p)], sems.at[p]))
        for copy in copies:
            copy.wait()

    return kernel


def scale_edge(parts):
    def kernel(q3a, q3b, *rest):
        stats, (_, out, buffers, sems) = rest[:parts], rest[parts:]
        mean, scale = scaled(parts, 0, stats)
        copies = []
        for h, q in enumerate((q3a, q3b)):
            scale_rows(q, mean, scale, buffers.at[h])
            copies.append(start(buffers.at[h], out.at[row_of(3), pl.ds(h * HALF, HALF)], sems.at[h]))
        for copy in copies:
            copy.wait()

    return kernel


def shards(tracer, c, s):
    lats, lons = (lax.axis_size(a) for a in ("lat", "lon"))
    on_pairs = [(i, i ^ 1) for i in range(lats)]
    cross_pairs = [(i, (((i + 1) ^ 1) - 1) % lats) for i in range(lats)]

    def rotated(array, axis, by):
        n = lax.axis_size(axis)
        return lax.ppermute(array, axis, [(i, (i + by) % n) for i in range(n)])

    def of_everyone(array):
        return [array] + [rotated(array, "lon", by) for by in range(1, lons)]

    def exchanged(faces):
        lon_low, lon_high, lev_low, lev_high = faces
        lev = (rotated(lev_high, "lev", 1), rotated(lev_low, "lev", -1))
        return [rotated(lon_high, "lon", 1), rotated(lon_low, "lon", -1), *lev]

    def swapped(q, pairs):
        return lax.ppermute(q, "lat", pairs)

    vm = lambda *arrays: [(a, VMEM) for a in arrays]
    dma = pltpu.SemaphoreType.DMA
    half, plane, face_outs = ((HALF_PLANE, VMEM), (PLANE, VMEM), [(f, VMEM) for f in FACES])
    inner_fields = ((3, *PLANE), VMEM)

    (x3a,) = call(first, [(tracer, HBM)], [half], scratch=[dma(())])
    x3b, x0, *faces = call(messages, [(tracer, HBM)], [half, plane] + face_outs, scratch=[dma((2 + 4 * NJ,))])
    cross = [swapped(x3a, cross_pairs), swapped(x3b, cross_pairs)]
    on = swapped(x0, on_pairs)
    halo = exchanged(faces)
    x2, c3, s3 = call(load_edge, [(a, HBM) for a in (tracer, c, s)], [plane] * 3, scratch=[dma((3,))])

    for step in range(STEPS):
        edge = vm(x2, x3a, x3b)
        rest = vm(*halo, c3, s3)
        if step < STEPS - 1:
            qa, *faces = call(edge_a, edge + vm(cross[0]) + rest, [half] + face_outs)
            cross[0] = swapped(qa, cross_pairs)
            outs = [plane] * 3 + face_outs
            if step == 0:
                q0, q1, q2, *faces, cc, ss = call(
                    inner_first,
                    [(a, HBM) for a in (tracer, c, s)] + vm(x0, x2, x3a, x3b, on, *halo, *faces),
                    outs + [inner_fields] * 2, scratch=[pltpu.VMEM(PLANE, F32), dma((7,))],
                    aliases={12 + n: 3 + n for n in range(4)}, limit=6 << 20,
                )
            else:
                q0, q1, q2, *faces = call(
                    inner, vm(x0, x1, x2, x3a, x3b, on, *halo, cc, ss, *faces), outs,
                    aliases={12 + n: 3 + n for n in range(4)},
                )
            on = swapped(q0, on_pairs)
            qb, *faces = call(
                edge_b, edge + vm(cross[1]) + rest + vm(*faces), [half] + face_outs,
                aliases={10 + n: 1 + n for n in range(4)},
            )
            cross[1] = swapped(qb, cross_pairs)
            halo = exchanged(faces)
        else:
            qa, raw = call(edge_a_last, edge + vm(cross[0]) + rest, [half, ((3, NK, NM), VMEM)])
            q0, q1, q2, stats, end = call(
                inner_last, vm(x0, x1, x2, x3a, x3b, on, *halo, cc, ss, raw),
                [plane] * 3 + [((2, 3, NK, NM), VMEM), ((NJ, *PLANE), HBM)], scratch=[dma((3,))],
            )
            inner_stats = of_everyone(stats)
            qb, stats = call(edge_b_last, edge + vm(cross[1]) + rest + vm(raw), [half, ((2, 1, NK, NM), VMEM)])
            edge_stats = of_everyone(stats)
        x0, x1, x2, x3a, x3b = q0, q1, q2, qa, qb

    out, end = call(
        scale_inner(lons), vm(x0, x1, x2, x3a, x3b, *inner_stats) + [(end, HBM)],
        [((NJ, *PLANE), HBM)] * 2, scratch=[pltpu.VMEM((3, *PLANE), F32), dma((5,))],
        aliases={5 + lons: 1}, limit=10 << 20,
    )
    (out,) = call(
        scale_edge(lons), vm(x3a, x3b, *edge_stats) + [(out, HBM)], [((NJ, *PLANE), HBM)],
        scratch=[pltpu.VMEM((2, *HALF_PLANE), F32), dma((2,))], aliases={2 + lons: 0}, limit=6 << 20,
    )
    return out, end


def solution(mesh):
    placed = P("lat", "lon", "lev", None)

    return jax.shard_map(
        shards, mesh=mesh, in_specs=(placed, placed, placed), out_specs=(placed, placed), check_vma=False
    )
```

```python
import jax
import jax.numpy as jnp
from jax import lax
from jax.experimental import pallas as pl
from jax.experimental.pallas import tpu as pltpu
from jax.sharding import PartitionSpec as P


STEPS = 3
F32 = jnp.float32
VMEM = pltpu.MemorySpace.VMEM
HBM = pltpu.MemorySpace.HBM
NJ, NI, NK, NM = 4, 128, 32, 128
HALF = NI // 2
PLANE = (NI, NK, NM)
HALF_PLANE = (HALF, NK, NM)
FACES = ((NJ, NK, NM),) * 2 + ((NJ, NI, NM),) * 2
UNROLL = 8
PIECE = 16


def call(kernel, args, outs, scratch=(), aliases=None, limit=4 << 20):
    arrays, in_specs = [], []
    for array, space in args:
        in_specs.append(pl.BlockSpec(memory_space=pl.ANY if space is HBM else space))
        arrays.append(pltpu.with_memory_space_constraint(array, space))
    return pl.pallas_call(
        kernel,
        out_shape=tuple(space(shape, F32) for shape, space in outs),
        in_specs=in_specs,
        out_specs=tuple(pl.BlockSpec(memory_space=pl.ANY if space is HBM else space) for _, space in outs),
        scratch_shapes=list(scratch),
        input_output_aliases=aliases or {},
        compiler_params=pltpu.CompilerParams(vmem_limit_bytes=limit),
    )(*arrays)


def row_of(p):
    odd = lax.rem(lax.axis_index("lat"), 2)
    return odd * p + (1 - odd) * (NJ - 1 - p)


def at_end(axis, high):
    return lax.axis_index(axis) == (lax.axis_size(axis) - 1 if high else 0)


def unless(outside, values):
    return jnp.where(outside, jnp.zeros_like(values), values)


def start(src, dst, sem):
    copy = pltpu.make_async_copy(src, dst, sem)
    copy.start()
    return copy


def first(tracer, x3a, sems):
    rows = [pl.ds(n, HALF // 4) for n in range(0, HALF, HALF // 4)]
    copies = [start(tracer.at[row_of(3), r], x3a.at[r], sems.at[n]) for n, r in enumerate(rows)]
    for copy in copies:
        copy.wait()


def messages(tracer, x3b, x0, lon_low, lon_high, lev_low, lev_high, sems):
    pairs = [
        (tracer.at[row_of(3), pl.ds(HALF, HALF)], x3b),
        (tracer.at[row_of(0)], x0),
    ]
    for p in range(NJ):
        j = row_of(p)
        pairs += [
            (tracer.at[j, :, 0, :], lev_low.at[p]),
            (tracer.at[j, :, NK - 1, :], lev_high.at[p]),
            (tracer.at[j, 0], lon_low.at[p]),
            (tracer.at[j, NI - 1], lon_high.at[p]),
        ]
    copies = [start(src, dst, sems.at[n]) for n, (src, dst) in enumerate(pairs)]
    for copy in copies:
        copy.wait()


def load_edge(tracer, c, s, x2, c3, s3, sems):
    pairs = [(tracer.at[row_of(2)], x2), (c.at[row_of(3)], c3), (s.at[row_of(3)], s3)]
    copies = [start(src, dst, sems.at[n]) for n, (src, dst) in enumerate(pairs)]
    for copy in copies:
        copy.wait()


def advance(x, before, after, below, above, lev_low, lev_high, c, s, out, lev_outs=None, sums=None, top=False):
    def at(view, i, size=None):
        ref, first = view
        return ref[first + i] if size is None else ref[pl.ds(pl.multiple_of(first + i, UNROLL), size), :]

    def block(b, carry):
        i0 = b * UNROLL
        low = unless(at_end("lev", False), at(lev_low, i0, UNROLL))
        high = unless(at_end("lev", True), at(lev_high, i0, UNROLL))
        prev = jnp.where(b == 0, before, at(x, jnp.maximum(i0 - 1, 0)))
        here = at(x, i0)
        for r in range(UNROLL):
            if r < UNROLL - 1:
                nxt = at(x, i0 + r + 1)
            else:
                nxt = jnp.where(b == HALF // UNROLL - 1, after, at(x, jnp.minimum(i0 + UNROLL, HALF - 1)))
            down = jnp.concatenate([low[r : r + 1], here[: NK - 1]], axis=0)
            up = jnp.concatenate([here[1:], high[r : r + 1]], axis=0)
            over = at(above, i0 + r) if top is False else unless(top, at(above, i0 + r))
            spread = (prev + nxt) + (at(below, i0 + r) + over) + (down + up) - 6.0 * here
            new = here + at(c, i0 + r) * spread + at(s, i0 + r)
            out[0][out[1] + i0 + r] = new
            if lev_outs is not None:
                for (ref, first), k in zip(lev_outs, (0, NK - 1)):
                    ref[pl.ds(first + i0 + r, 1), :] = new[k : k + 1]
            if sums is not None:
                shift, total, squares = carry
                if r == 0 and sums[0] is None:
                    shift = jnp.where(b == 0, new, shift)
                moved = new - shift
                carry = (shift, total + moved, squares + moved * moved)
            prev, here = here, nxt
        return carry

    if sums is None:
        first = 0
    else:
        first = (jnp.zeros((NK, NM), F32) if sums[0] is None else sums[0], *sums[1:])
    return lax.fori_loop(0, HALF // UNROLL, block, first)


def put_stats(stats, p, sums):
    shift, total, squares = sums
    stats[0, p] = shift + total * (1.0 / NI)
    stats[1, p] = squares - total * (total * (1.0 / NI))


def no_sums():
    zero = jnp.zeros((NK, NM), F32)
    return (None, zero, zero)


def inner_planes(xs, on, halo, cs, outs, faces=None, stats=None, ready=lambda p: None, done=lambda p, h: None):
    lon_low, lon_high, lev_low, lev_high = halo
    for p in (2, 1, 0):
        ready(p)
        x, out = xs[p], outs[p]
        sums = no_sums() if stats is not None else None
        for h in (0, 1):
            first = h * HALF
            below = (on, first) if p == 0 else (xs[p - 1], first)
            above = (xs[3 + h], 0) if p == 2 else (xs[p + 1], first)
            before = x[HALF - 1] if h else unless(at_end("lon", False), lon_low[p])
            after = unless(at_end("lon", True), lon_high[p]) if h else x[HALF]
            sums = advance(
                (x, first), before, after, below, above, (lev_low.at[p], first), (lev_high.at[p], first),
                (cs[p][0], first), (cs[p][1], first), (out, first),
                None if faces is None else ((faces[2].at[p], first), (faces[3].at[p], first)),
                sums if stats is not None else None,
            )
            done(p, h)
        if faces is not None:
            faces[0][p] = out[0]
            faces[1][p] = out[NI - 1]
        if stats is not None:
            put_stats(stats, p, sums)


def edge_half(h, x2, x3, cross, halo, c3, s3, out, faces=None, sums=None):
    lon_low, lon_high, lev_low, lev_high = halo
    p, first = 3, h * HALF
    before = x3[0][HALF - 1] if h else unless(at_end("lon", False), lon_low[p])
    after = unless(at_end("lon", True), lon_high[p]) if h else x3[1][0]
    sums = advance(
        (x3[h], 0), before, after,
        (x2, first), (cross, 0), (lev_low.at[p], first), (lev_high.at[p], first), (c3, first), (s3, first), (out, 0),
        None if faces is None else ((faces[2].at[p], first), (faces[3].at[p], first)), sums,
        jnp.logical_or(at_end("lat", False), at_end("lat", True)),
    )
    if faces is not None:
        if h:
            faces[1][p] = out[HALF - 1]
        else:
            faces[0][p] = out[0]
    return sums


def edge_a(x2, x3a, x3b, cross, ll, lh, vl, vh, c3, s3, out, *faces):
    edge_half(0, x2, (x3a, x3b), cross, (ll, lh, vl, vh), c3, s3, out, faces)


def edge_b(x2, x3a, x3b, cross, ll, lh, vl, vh, c3, s3, a0, a1, a2, a3, out, *faces):
    edge_half(1, x2, (x3a, x3b), cross, (ll, lh, vl, vh), c3, s3, out, faces)


def edge_a_last(x2, x3a, x3b, cross, ll, lh, vl, vh, c3, s3, out, raw):
    sums = edge_half(0, x2, (x3a, x3b), cross, (ll, lh, vl, vh), c3, s3, out, None, no_sums())
    for n in range(3):
        raw[n] = sums[n]


def edge_b_last(x2, x3a, x3b, cross, ll, lh, vl, vh, c3, s3, raw, out, stats):
    sums = (raw[0], raw[1], raw[2])
    put_stats(stats, 0, edge_half(1, x2, (x3a, x3b), cross, (ll, lh, vl, vh), c3, s3, out, None, sums))


def inner_first(
    tracer, c, s, x0, x2, x3a, x3b, on, ll, lh, vl, vh, a0, a1, a2, a3, q0, q1, q2, f0, f1, f2, f3, cc, ss, x1, sems
):
    loads = [[start(tracer.at[row_of(1)], x1, sems.at[6])], [], []]
    for p in (2, 1, 0):
        loads[p] += [start(c.at[row_of(p)], cc.at[p], sems.at[p]), start(s.at[row_of(p)], ss.at[p], sems.at[3 + p])]
    loads[2] += loads[0][:1]
    loads[0] = loads[0][1:]

    def ready(p):
        for copy in loads[p]:
            copy.wait()

    inner_planes(
        (x0, x1, x2, x3a, x3b), on, (ll, lh, vl, vh), [(cc.at[p], ss.at[p]) for p in range(3)], (q0, q1, q2),
        (f0, f1, f2, f3), ready=ready,
    )


def inner(x0, x1, x2, x3a, x3b, on, ll, lh, vl, vh, cc, ss, a0, a1, a2, a3, q0, q1, q2, *faces):
    inner_planes(
        (x0, x1, x2, x3a, x3b), on, (ll, lh, vl, vh), [(cc.at[p], ss.at[p]) for p in range(3)], (q0, q1, q2), faces
    )


def inner_last(x0, x1, x2, x3a, x3b, on, ll, lh, vl, vh, cc, ss, q0, q1, q2, stats, end, sems):
    outs, copies = ((q0, q1, q2), [])

    def done(p, h):
        rows = pl.ds(h * HALF, HALF)
        copies.append(start(outs[p].at[rows], end.at[row_of(p), rows], sems.at[2 * p + h]))

    inner_planes(
        (x0, x1, x2, x3a, x3b), on, (ll, lh, vl, vh), [(cc.at[p], ss.at[p]) for p in range(3)], outs, None, stats,
        done=done,
    )
    for copy in copies:
        copy.wait()


def scaled(parts, p, stats):
    means = [part[0, p] for part in stats]
    mean = sum(means[1:], means[0]) * (1.0 / parts)
    square = sum([part[1, p] for part in stats[1:]], stats[0][1, p])
    for m in means:
        square = square + NI * ((m - mean) * (m - mean))
    return mean, lax.rsqrt(square * (1.0 / (parts * NI)) + 0.0001)


def scale_rows(q, mean, scale, out):
    def block(b, _):
        i0 = b * UNROLL
        for r in range(UNROLL):
            out[i0 + r] = (q[i0 + r] - mean) * scale
        return 0

    lax.fori_loop(0, q.shape[0] // UNROLL, block, 0)


def scale_inner(parts):
    def kernel(q0, q1, q2, q3a, q3b, *rest):
        stats, (_, out, end, buffers, sems) = rest[:parts], rest[parts:]
        copies = [start(q, end.at[row_of(3), pl.ds(h * HALF, HALF)], sems.at[3 + h]) for h, q in enumerate((q3a, q3b))]
        for p, q in enumerate((q0, q1, q2)):
            scale_rows(q, *scaled(parts, p, stats), buffers.at[p])
            copies.append(start(buffers.at[p], out.at[row_of(p)], sems.at[p]))
        for copy in copies:
            copy.wait()

    return kernel


def scale_edge(parts):
    def kernel(q3a, q3b, *rest):
        stats, (_, out, buffer, sems) = rest[:parts], rest[parts:]
        mean, scale = scaled(parts, 0, stats)
        copies = []
        for h, q in enumerate((q3a, q3b)):
            for first in range(0, HALF, PIECE):
                rows = pl.ds(h * HALF + first, PIECE)
                scale_rows(q.at[pl.ds(first, PIECE)], mean, scale, buffer.at[rows])
                copies.append(start(buffer.at[rows], out.at[row_of(3), rows], sems.at[len(copies)]))
        for copy in copies:
            copy.wait()

    return kernel


def turns(n):
    return range(n - 1, 0, -1)


def shards(tracer, c, s):
    lats, lons = (lax.axis_size(a) for a in ("lat", "lon"))
    on_pairs = [(i, i ^ 1) for i in range(lats)]
    cross_pairs = [(i, (((i + 1) ^ 1) - 1) % lats) for i in range(lats)]
    inside_pairs = cross_pairs[1:-1]

    def rotated(array, axis, by):
        n = lax.axis_size(axis)
        return lax.ppermute(array, axis, [(i, (i + by) % n) for i in range(n)])

    def of_everyone(array):
        return [array] + [rotated(array, "lon", by) for by in turns(lons)]

    def exchanged(faces):
        lon_low, lon_high, lev_low, lev_high = faces
        lev = (rotated(lev_high, "lev", 1), rotated(lev_low, "lev", -1))
        return [rotated(lon_high, "lon", 1), rotated(lon_low, "lon", -1), *lev]

    def swapped(q, pairs):
        return lax.ppermute(q, "lat", pairs)

    vm = lambda *arrays: [(a, VMEM) for a in arrays]
    dma = pltpu.SemaphoreType.DMA
    half, plane, face_outs = ((HALF_PLANE, VMEM), (PLANE, VMEM), [(f, VMEM) for f in FACES])
    inner_fields = ((3, *PLANE), VMEM)

    (x3a,) = call(first, [(tracer, HBM)], [half], scratch=[dma((4,))])
    x3b, x0, *faces = call(messages, [(tracer, HBM)], [half, plane] + face_outs, scratch=[dma((2 + 4 * NJ,))])
    cross = [swapped(x3a, cross_pairs), swapped(x3b, cross_pairs)]
    on = swapped(x0, on_pairs)
    halo = exchanged(faces)
    x2, c3, s3 = call(load_edge, [(a, HBM) for a in (tracer, c, s)], [plane] * 3, scratch=[dma((3,))])

    for step in range(STEPS):
        edge = vm(x2, x3a, x3b)
        rest = vm(*halo, c3, s3)
        if step < STEPS - 1:
            qa, *faces = call(edge_a, edge + vm(cross[0]) + rest, [half] + face_outs)
            cross[0] = swapped(qa, cross_pairs)
            outs = [plane] * 3 + face_outs
            if step == 0:
                q0, q1, q2, *faces, cc, ss = call(
                    inner_first,
                    [(a, HBM) for a in (tracer, c, s)] + vm(x0, x2, x3a, x3b, on, *halo, *faces),
                    outs + [inner_fields] * 2, scratch=[pltpu.VMEM(PLANE, F32), dma((7,))],
                    aliases={12 + n: 3 + n for n in range(4)}, limit=6 << 20,
                )
            else:
                q0, q1, q2, *faces = call(
                    inner, vm(x0, x1, x2, x3a, x3b, on, *halo, cc, ss, *faces), outs,
                    aliases={12 + n: 3 + n for n in range(4)},
                )
            on = swapped(q0, on_pairs)
            qb, *faces = call(
                edge_b, edge + vm(cross[1]) + rest + vm(*faces), [half] + face_outs,
                aliases={10 + n: 1 + n for n in range(4)},
            )
            cross[1] = swapped(qb, inside_pairs)
            halo = exchanged(faces)
        else:
            q0, q1, q2, stats, end = call(
                inner_last, vm(x0, x1, x2, x3a, x3b, on, *halo, cc, ss),
                [plane] * 3 + [((2, 3, NK, NM), VMEM), ((NJ, *PLANE), HBM)], scratch=[dma((6,))],
            )
            inner_stats = of_everyone(stats)
            qa, raw = call(edge_a_last, edge + vm(cross[0]) + rest, [half, ((3, NK, NM), VMEM)])
            qb, stats = call(edge_b_last, edge + vm(cross[1]) + rest + vm(raw), [half, ((2, 1, NK, NM), VMEM)])
            edge_stats = of_everyone(stats)
        x0, x1, x2, x3a, x3b = q0, q1, q2, qa, qb

    out, end = call(
        scale_inner(lons), vm(x0, x1, x2, x3a, x3b, *inner_stats) + [(end, HBM)],
        [((NJ, *PLANE), HBM)] * 2, scratch=[pltpu.VMEM((3, *PLANE), F32), dma((5,))],
        aliases={5 + lons: 1}, limit=10 << 20,
    )
    (out,) = call(
        scale_edge(lons), vm(x3a, x3b, *edge_stats) + [(out, HBM)], [((NJ, *PLANE), HBM)],
        scratch=[pltpu.VMEM(PLANE, F32), dma((NI // PIECE,))], aliases={2 + lons: 0}, limit=6 << 20,
    )
    return out, end


def solution(mesh):
    placed = P("lat", "lon", "lev", None)

    return jax.shard_map(
        shards, mesh=mesh, in_specs=(placed, placed, placed), out_specs=(placed, placed), check_vma=False
    )
```

```python
import jax
import jax.numpy as jnp
from jax import lax
from jax.experimental import pallas as pl
from jax.experimental.pallas import tpu as pltpu
from jax.sharding import PartitionSpec as P


STEPS = 3
F32 = jnp.float32
VMEM = pltpu.MemorySpace.VMEM
HBM = pltpu.MemorySpace.HBM
NJ, NI, NK, NM = 4, 128, 32, 128
HALF = NI // 2
PLANE = (NI, NK, NM)
HALF_PLANE = (HALF, NK, NM)
FACES = ((NJ, NK, NM),) * 2 + ((NJ, NI, NM),) * 2
UNROLL = 8
PIECE = 16


def call(kernel, args, outs, scratch=(), aliases=None, limit=4 << 20):
    arrays, in_specs = [], []
    for array, space in args:
        in_specs.append(pl.BlockSpec(memory_space=pl.ANY if space is HBM else space))
        arrays.append(pltpu.with_memory_space_constraint(array, space))
    return pl.pallas_call(
        kernel,
        out_shape=tuple(space(shape, F32) for shape, space in outs),
        in_specs=in_specs,
        out_specs=tuple(pl.BlockSpec(memory_space=pl.ANY if space is HBM else space) for _, space in outs),
        scratch_shapes=list(scratch),
        input_output_aliases=aliases or {},
        compiler_params=pltpu.CompilerParams(vmem_limit_bytes=limit),
    )(*arrays)


def row_of(p):
    odd = lax.rem(lax.axis_index("lat"), 2)
    return odd * p + (1 - odd) * (NJ - 1 - p)


def at_end(axis, high):
    return lax.axis_index(axis) == (lax.axis_size(axis) - 1 if high else 0)


def unless(outside, values):
    return jnp.where(outside, jnp.zeros_like(values), values)


def start(src, dst, sem):
    copy = pltpu.make_async_copy(src, dst, sem)
    copy.start()
    return copy


def first(tracer, x3a, sems):
    rows = [pl.ds(n, HALF // 4) for n in range(0, HALF, HALF // 4)]
    copies = [start(tracer.at[row_of(3), r], x3a.at[r], sems.at[n]) for n, r in enumerate(rows)]
    for copy in copies:
        copy.wait()


def messages(tracer, x3b, x0, lon_low, lon_high, lev_low, lev_high, sems):
    pairs = [
        (tracer.at[row_of(3), pl.ds(HALF, HALF)], x3b),
        (tracer.at[row_of(0)], x0),
    ]
    for p in range(NJ):
        j = row_of(p)
        pairs += [
            (tracer.at[j, :, 0, :], lev_low.at[p]),
            (tracer.at[j, :, NK - 1, :], lev_high.at[p]),
            (tracer.at[j, 0], lon_low.at[p]),
            (tracer.at[j, NI - 1], lon_high.at[p]),
        ]
    copies = [start(src, dst, sems.at[n]) for n, (src, dst) in enumerate(pairs)]
    for copy in copies:
        copy.wait()


def load_edge(tracer, c, s, x2, c3, s3, sems):
    pairs = [(tracer.at[row_of(2)], x2), (c.at[row_of(3)], c3), (s.at[row_of(3)], s3)]
    copies = [start(src, dst, sems.at[n]) for n, (src, dst) in enumerate(pairs)]
    for copy in copies:
        copy.wait()


def advance(x, before, after, below, above, lev_low, lev_high, c, s, out, lev_outs=None, sums=None, top=False):
    def at(view, i, size=None):
        ref, first = view
        return ref[first + i] if size is None else ref[pl.ds(pl.multiple_of(first + i, UNROLL), size), :]

    def block(b, carry):
        i0 = b * UNROLL
        low = unless(at_end("lev", False), at(lev_low, i0, UNROLL))
        high = unless(at_end("lev", True), at(lev_high, i0, UNROLL))
        prev = jnp.where(b == 0, before, at(x, jnp.maximum(i0 - 1, 0)))
        here = at(x, i0)
        for r in range(UNROLL):
            if r < UNROLL - 1:
                nxt = at(x, i0 + r + 1)
            else:
                nxt = jnp.where(b == HALF // UNROLL - 1, after, at(x, jnp.minimum(i0 + UNROLL, HALF - 1)))
            down = jnp.concatenate([low[r : r + 1], here[: NK - 1]], axis=0)
            up = jnp.concatenate([here[1:], high[r : r + 1]], axis=0)
            over = at(above, i0 + r) if top is False else unless(top, at(above, i0 + r))
            spread = (prev + nxt) + (at(below, i0 + r) + over) + (down + up) - 6.0 * here
            new = here + at(c, i0 + r) * spread + at(s, i0 + r)
            out[0][out[1] + i0 + r] = new
            if lev_outs is not None:
                for (ref, first), k in zip(lev_outs, (0, NK - 1)):
                    ref[pl.ds(first + i0 + r, 1), :] = new[k : k + 1]
            if sums is not None:
                shift, total = carry
                if r == 0 and sums[0] is None:
                    shift = jnp.where(b == 0, new, shift)
                carry = (shift, total + (new - shift))
            prev, here = here, nxt
        return carry

    if sums is None:
        first = 0
    else:
        first = (jnp.zeros((NK, NM), F32) if sums[0] is None else sums[0], sums[1])
    return lax.fori_loop(0, HALF // UNROLL, block, first)


def moments(q, sums):
    shift, total = sums
    rows = q.shape[0]
    mean = shift + total * (1.0 / rows)

    def block(b, squares):
        for r in range(UNROLL):
            moved = q[b * UNROLL + r] - mean
            squares = squares + moved * moved
        return squares

    return mean, lax.fori_loop(0, rows // UNROLL, block, jnp.zeros((NK, NM), F32))


def no_sums():
    return (None, jnp.zeros((NK, NM), F32))


def inner_planes(xs, on, halo, cs, outs, faces=None, stats=None, ready=lambda p: None, done=lambda p, h: None):
    lon_low, lon_high, lev_low, lev_high = halo
    for p in (2, 1, 0):
        ready(p)
        x, out = xs[p], outs[p]
        sums = no_sums() if stats is not None else None
        for h in (0, 1):
            first = h * HALF
            below = (on, first) if p == 0 else (xs[p - 1], first)
            above = (xs[3 + h], 0) if p == 2 else (xs[p + 1], first)
            before = x[HALF - 1] if h else unless(at_end("lon", False), lon_low[p])
            after = unless(at_end("lon", True), lon_high[p]) if h else x[HALF]
            sums = advance(
                (x, first), before, after, below, above, (lev_low.at[p], first), (lev_high.at[p], first),
                (cs[p][0], first), (cs[p][1], first), (out, first),
                None if faces is None else ((faces[2].at[p], first), (faces[3].at[p], first)),
                sums if stats is not None else None,
            )
            done(p, h)
        if faces is not None:
            faces[0][p] = out[0]
            faces[1][p] = out[NI - 1]
        if stats is not None:
            stats[0, p], stats[1, p] = moments(out, sums)


def edge_half(h, x2, x3, cross, halo, c3, s3, out, faces=None, sums=None):
    lon_low, lon_high, lev_low, lev_high = halo
    p, first = 3, h * HALF
    before = x3[0][HALF - 1] if h else unless(at_end("lon", False), lon_low[p])
    after = unless(at_end("lon", True), lon_high[p]) if h else x3[1][0]
    sums = advance(
        (x3[h], 0), before, after,
        (x2, first), (cross, 0), (lev_low.at[p], first), (lev_high.at[p], first), (c3, first), (s3, first), (out, 0),
        None if faces is None else ((faces[2].at[p], first), (faces[3].at[p], first)), sums,
        jnp.logical_or(at_end("lat", False), at_end("lat", True)),
    )
    if faces is not None:
        if h:
            faces[1][p] = out[HALF - 1]
        else:
            faces[0][p] = out[0]
    return sums


def edge_a(x2, x3a, x3b, cross, ll, lh, vl, vh, c3, s3, out, *faces):
    edge_half(0, x2, (x3a, x3b), cross, (ll, lh, vl, vh), c3, s3, out, faces)


def edge_b(x2, x3a, x3b, cross, ll, lh, vl, vh, c3, s3, a0, a1, a2, a3, out, *faces):
    edge_half(1, x2, (x3a, x3b), cross, (ll, lh, vl, vh), c3, s3, out, faces)


def edge_a_last(x2, x3a, x3b, cross, ll, lh, vl, vh, c3, s3, out, raw):
    raw[0], raw[1] = moments(out, edge_half(0, x2, (x3a, x3b), cross, (ll, lh, vl, vh), c3, s3, out, None, no_sums()))


def edge_b_last(x2, x3a, x3b, cross, ll, lh, vl, vh, c3, s3, raw, out, stats):
    mean, square = moments(out, edge_half(1, x2, (x3a, x3b), cross, (ll, lh, vl, vh), c3, s3, out, None, no_sums()))
    stats[0, 0] = 0.5 * (raw[0] + mean)
    stats[1, 0] = raw[1] + square + (0.5 * HALF) * ((raw[0] - mean) * (raw[0] - mean))


def inner_first(
    tracer, c, s, x0, x2, x3a, x3b, on, ll, lh, vl, vh, a0, a1, a2, a3, q0, q1, q2, f0, f1, f2, f3, cc, ss, x1, sems
):
    loads = [[start(tracer.at[row_of(1)], x1, sems.at[6])], [], []]
    for p in (2, 1, 0):
        loads[p] += [start(c.at[row_of(p)], cc.at[p], sems.at[p]), start(s.at[row_of(p)], ss.at[p], sems.at[3 + p])]
    loads[2] += loads[0][:1]
    loads[0] = loads[0][1:]

    def ready(p):
        for copy in loads[p]:
            copy.wait()

    inner_planes(
        (x0, x1, x2, x3a, x3b), on, (ll, lh, vl, vh), [(cc.at[p], ss.at[p]) for p in range(3)], (q0, q1, q2),
        (f0, f1, f2, f3), ready=ready,
    )


def inner(x0, x1, x2, x3a, x3b, on, ll, lh, vl, vh, cc, ss, a0, a1, a2, a3, q0, q1, q2, *faces):
    inner_planes(
        (x0, x1, x2, x3a, x3b), on, (ll, lh, vl, vh), [(cc.at[p], ss.at[p]) for p in range(3)], (q0, q1, q2), faces
    )


def inner_last(x0, x1, x2, x3a, x3b, on, ll, lh, vl, vh, cc, ss, q0, q1, q2, stats, end, sems):
    outs, copies = ((q0, q1, q2), [])

    def done(p, h):
        rows = pl.ds(h * HALF, HALF)
        copies.append(start(outs[p].at[rows], end.at[row_of(p), rows], sems.at[2 * p + h]))

    inner_planes(
        (x0, x1, x2, x3a, x3b), on, (ll, lh, vl, vh), [(cc.at[p], ss.at[p]) for p in range(3)], outs, None, stats,
        done=done,
    )
    for copy in copies:
        copy.wait()


def scaled(parts, p, stats):
    means = [part[0, p] for part in stats]
    mean = sum(means[1:], means[0]) * (1.0 / parts)
    square = sum([part[1, p] for part in stats[1:]], stats[0][1, p])
    for m in means:
        square = square + NI * ((m - mean) * (m - mean))
    return mean, lax.rsqrt(square * (1.0 / (parts * NI)) + 0.0001)


def scale_rows(q, mean, scale, out):
    def block(b, _):
        i0 = b * UNROLL
        for r in range(UNROLL):
            out[i0 + r] = (q[i0 + r] - mean) * scale
        return 0

    lax.fori_loop(0, q.shape[0] // UNROLL, block, 0)


def scale_inner(parts):
    def kernel(q0, q1, q2, q3a, q3b, *rest):
        stats, (_, out, end, buffers, sems) = rest[:parts], rest[parts:]
        copies = [start(q, end.at[row_of(3), pl.ds(h * HALF, HALF)], sems.at[3 + h]) for h, q in enumerate((q3a, q3b))]
        for p, q in enumerate((q0, q1, q2)):
            scale_rows(q, *scaled(parts, p, stats), buffers.at[p])
            copies.append(start(buffers.at[p], out.at[row_of(p)], sems.at[p]))
        for copy in copies:
            copy.wait()

    return kernel


def scale_edge(parts):
    def kernel(q3a, q3b, *rest):
        stats, (_, out, buffer, sems) = rest[:parts], rest[parts:]
        mean, scale = scaled(parts, 0, stats)
        copies = []
        for h, q in enumerate((q3a, q3b)):
            for first in range(0, HALF, PIECE):
                rows = pl.ds(h * HALF + first, PIECE)
                scale_rows(q.at[pl.ds(first, PIECE)], mean, scale, buffer.at[rows])
                copies.append(start(buffer.at[rows], out.at[row_of(3), rows], sems.at[len(copies)]))
        for copy in copies:
            copy.wait()

    return kernel


def turns(n):
    return range(n - 1, 0, -1)


def shards(tracer, c, s):
    lats, lons = (lax.axis_size(a) for a in ("lat", "lon"))
    on_pairs = [(i, i ^ 1) for i in range(lats)]
    cross_pairs = [(i, (((i + 1) ^ 1) - 1) % lats) for i in range(lats)]
    inside_pairs = cross_pairs[1:-1]

    def rotated(array, axis, by):
        n = lax.axis_size(axis)
        return lax.ppermute(array, axis, [(i, (i + by) % n) for i in range(n)])

    def of_everyone(array):
        return [array] + [rotated(array, "lon", by) for by in turns(lons)]

    def exchanged(faces):
        lon_low, lon_high, lev_low, lev_high = faces
        lev = (rotated(lev_high, "lev", 1), rotated(lev_low, "lev", -1))
        return [rotated(lon_high, "lon", 1), rotated(lon_low, "lon", -1), *lev]

    def swapped(q, pairs):
        return lax.ppermute(q, "lat", pairs)

    vm = lambda *arrays: [(a, VMEM) for a in arrays]
    dma = pltpu.SemaphoreType.DMA
    half, plane, face_outs = ((HALF_PLANE, VMEM), (PLANE, VMEM), [(f, VMEM) for f in FACES])
    inner_fields = ((3, *PLANE), VMEM)

    (x3a,) = call(first, [(tracer, HBM)], [half], scratch=[dma((4,))])
    x3b, x0, *faces = call(messages, [(tracer, HBM)], [half, plane] + face_outs, scratch=[dma((2 + 4 * NJ,))])
    cross = [swapped(x3a, cross_pairs), swapped(x3b, cross_pairs)]
    on = swapped(x0, on_pairs)
    halo = exchanged(faces)
    x2, c3, s3 = call(load_edge, [(a, HBM) for a in (tracer, c, s)], [plane] * 3, scratch=[dma((3,))])

    for step in range(STEPS):
        edge = vm(x2, x3a, x3b)
        rest = vm(*halo, c3, s3)
        if step < STEPS - 1:
            qa, *faces = call(edge_a, edge + vm(cross[0]) + rest, [half] + face_outs)
            cross[0] = swapped(qa, cross_pairs)
            outs = [plane] * 3 + face_outs
            if step == 0:
                q0, q1, q2, *faces, cc, ss = call(
                    inner_first,
                    [(a, HBM) for a in (tracer, c, s)] + vm(x0, x2, x3a, x3b, on, *halo, *faces),
                    outs + [inner_fields] * 2, scratch=[pltpu.VMEM(PLANE, F32), dma((7,))],
                    aliases={12 + n: 3 + n for n in range(4)}, limit=6 << 20,
                )
            else:
                q0, q1, q2, *faces = call(
                    inner, vm(x0, x1, x2, x3a, x3b, on, *halo, cc, ss, *faces), outs,
                    aliases={12 + n: 3 + n for n in range(4)},
                )
            on = swapped(q0, on_pairs)
            qb, *faces = call(
                edge_b, edge + vm(cross[1]) + rest + vm(*faces), [half] + face_outs,
                aliases={10 + n: 1 + n for n in range(4)},
            )
            cross[1] = swapped(qb, inside_pairs)
            halo = exchanged(faces)
        else:
            q0, q1, q2, stats, end = call(
                inner_last, vm(x0, x1, x2, x3a, x3b, on, *halo, cc, ss),
                [plane] * 3 + [((2, 3, NK, NM), VMEM), ((NJ, *PLANE), HBM)], scratch=[dma((6,))],
            )
            inner_stats = of_everyone(stats)
            qa, raw = call(edge_a_last, edge + vm(cross[0]) + rest, [half, ((2, NK, NM), VMEM)])
            qb, stats = call(edge_b_last, edge + vm(cross[1]) + rest + vm(raw), [half, ((2, 1, NK, NM), VMEM)])
            edge_stats = of_everyone(stats)
        x0, x1, x2, x3a, x3b = q0, q1, q2, qa, qb

    out, end = call(
        scale_inner(lons), vm(x0, x1, x2, x3a, x3b, *inner_stats) + [(end, HBM)],
        [((NJ, *PLANE), HBM)] * 2, scratch=[pltpu.VMEM((3, *PLANE), F32), dma((5,))],
        aliases={5 + lons: 1}, limit=10 << 20,
    )
    (out,) = call(
        scale_edge(lons), vm(x3a, x3b, *edge_stats) + [(out, HBM)], [((NJ, *PLANE), HBM)],
        scratch=[pltpu.VMEM(PLANE, F32), dma((NI // PIECE,))], aliases={2 + lons: 0}, limit=6 << 20,
    )
    return out, end


def solution(mesh):
    placed = P("lat", "lon", "lev", None)

    return jax.shard_map(
        shards, mesh=mesh, in_specs=(placed, placed, placed), out_specs=(placed, placed), check_vma=False
    )
```

```python
import jax
import jax.numpy as jnp
from jax import lax
from jax.experimental import pallas as pl
from jax.experimental.pallas import tpu as pltpu
from jax.sharding import PartitionSpec as P


STEPS = 3
F32 = jnp.float32
VMEM = pltpu.MemorySpace.VMEM
HBM = pltpu.MemorySpace.HBM
NJ, NI, NK, NM = 4, 128, 32, 128
CUTS = ((0, 80), (80, 48))
PLANE = (NI, NK, NM)
PARTS = tuple((rows, NK, NM) for _, rows in CUTS)
FACES = ((NJ, NK, NM),) * 2 + ((NJ, NI, NM),) * 2
UNROLL = 8
PIECE = 16


def call(kernel, args, outs, scratch=(), aliases=None, limit=4 << 20):
    arrays, in_specs = [], []
    for array, space in args:
        in_specs.append(pl.BlockSpec(memory_space=pl.ANY if space is HBM else space))
        arrays.append(pltpu.with_memory_space_constraint(array, space))
    return pl.pallas_call(
        kernel,
        out_shape=tuple(space(shape, F32) for shape, space in outs),
        in_specs=in_specs,
        out_specs=tuple(pl.BlockSpec(memory_space=pl.ANY if space is HBM else space) for _, space in outs),
        scratch_shapes=list(scratch),
        input_output_aliases=aliases or {},
        compiler_params=pltpu.CompilerParams(vmem_limit_bytes=limit),
    )(*arrays)


def row_of(p):
    odd = lax.rem(lax.axis_index("lat"), 2)
    return odd * p + (1 - odd) * (NJ - 1 - p)


def at_end(axis, high):
    return lax.axis_index(axis) == (lax.axis_size(axis) - 1 if high else 0)


def unless(outside, values):
    return jnp.where(outside, jnp.zeros_like(values), values)


def start(src, dst, sem):
    copy = pltpu.make_async_copy(src, dst, sem)
    copy.start()
    return copy


def first(tracer, x3a, sems):
    size = CUTS[0][1] // 4
    rows = [pl.ds(n * size, size) for n in range(4)]
    copies = [start(tracer.at[row_of(3), r], x3a.at[r], sems.at[n]) for n, r in enumerate(rows)]
    for copy in copies:
        copy.wait()


def messages(tracer, x3b, x0, lon_low, lon_high, lev_low, lev_high, sems):
    pairs = [
        (tracer.at[row_of(3), pl.ds(*CUTS[1])], x3b),
        (tracer.at[row_of(0)], x0),
    ]
    for p in range(NJ):
        j = row_of(p)
        pairs += [
            (tracer.at[j, :, 0, :], lev_low.at[p]),
            (tracer.at[j, :, NK - 1, :], lev_high.at[p]),
            (tracer.at[j, 0], lon_low.at[p]),
            (tracer.at[j, NI - 1], lon_high.at[p]),
        ]
    copies = [start(src, dst, sems.at[n]) for n, (src, dst) in enumerate(pairs)]
    for copy in copies:
        copy.wait()


def load_edge(tracer, c, s, x2, c3, s3, sems):
    pairs = [(tracer.at[row_of(2)], x2), (c.at[row_of(3)], c3), (s.at[row_of(3)], s3)]
    copies = [start(src, dst, sems.at[n]) for n, (src, dst) in enumerate(pairs)]
    for copy in copies:
        copy.wait()


def advance(rows, x, before, after, below, above, lev_low, lev_high, c, s, out, lev_outs=None, sums=None, top=False):
    def at(view, i, size=None):
        ref, first = view
        return ref[first + i] if size is None else ref[pl.ds(pl.multiple_of(first + i, UNROLL), size), :]

    def block(b, carry):
        i0 = b * UNROLL
        low = unless(at_end("lev", False), at(lev_low, i0, UNROLL))
        high = unless(at_end("lev", True), at(lev_high, i0, UNROLL))
        prev = jnp.where(b == 0, before, at(x, jnp.maximum(i0 - 1, 0)))
        here = at(x, i0)
        for r in range(UNROLL):
            if r < UNROLL - 1:
                nxt = at(x, i0 + r + 1)
            else:
                nxt = jnp.where(b == rows // UNROLL - 1, after, at(x, jnp.minimum(i0 + UNROLL, rows - 1)))
            down = jnp.concatenate([low[r : r + 1], here[: NK - 1]], axis=0)
            up = jnp.concatenate([here[1:], high[r : r + 1]], axis=0)
            over = at(above, i0 + r) if top is False else unless(top, at(above, i0 + r))
            spread = (prev + nxt) + (at(below, i0 + r) + over) + (down + up) - 6.0 * here
            new = here + at(c, i0 + r) * spread + at(s, i0 + r)
            out[0][out[1] + i0 + r] = new
            if lev_outs is not None:
                for (ref, first), k in zip(lev_outs, (0, NK - 1)):
                    ref[pl.ds(first + i0 + r, 1), :] = new[k : k + 1]
            if sums is not None:
                shift, total = carry
                if r == 0 and sums[0] is None:
                    shift = jnp.where(b == 0, new, shift)
                carry = (shift, total + (new - shift))
            prev, here = here, nxt
        return carry

    if sums is None:
        first = 0
    else:
        first = (jnp.zeros((NK, NM), F32) if sums[0] is None else sums[0], sums[1])
    return lax.fori_loop(0, rows // UNROLL, block, first)


def moments(q, sums):
    shift, total = sums
    rows = q.shape[0]
    mean = shift + total * (1.0 / rows)

    def block(b, squares):
        for r in range(UNROLL):
            moved = q[b * UNROLL + r] - mean
            squares = squares + moved * moved
        return squares

    return mean, lax.fori_loop(0, rows // UNROLL, block, jnp.zeros((NK, NM), F32))


def no_sums():
    return (None, jnp.zeros((NK, NM), F32))


def inner_planes(xs, on, halo, cs, outs, faces=None, stats=None, ready=lambda p: None, done=lambda p, h: None):
    lon_low, lon_high, lev_low, lev_high = halo
    for p in (2, 1, 0):
        ready(p)
        x, out = xs[p], outs[p]
        sums = no_sums() if stats is not None else None
        for h in (0, 1):
            first, rows = CUTS[h]
            below = (on, first) if p == 0 else (xs[p - 1], first)
            above = (xs[3 + h], 0) if p == 2 else (xs[p + 1], first)
            before = x[first - 1] if h else unless(at_end("lon", False), lon_low[p])
            after = unless(at_end("lon", True), lon_high[p]) if h else x[rows]
            sums = advance(
                rows,
                (x, first), before, after, below, above, (lev_low.at[p], first), (lev_high.at[p], first),
                (cs[p][0], first), (cs[p][1], first), (out, first),
                None if faces is None else ((faces[2].at[p], first), (faces[3].at[p], first)),
                sums if stats is not None else None,
            )
            done(p, h)
        if faces is not None:
            faces[0][p] = out[0]
            faces[1][p] = out[NI - 1]
        if stats is not None:
            stats[0, p], stats[1, p] = moments(out, sums)


def edge_half(h, x2, x3, cross, halo, c3, s3, out, faces=None, sums=None):
    lon_low, lon_high, lev_low, lev_high = halo
    p, (first, rows) = 3, CUTS[h]
    before = x3[0][first - 1] if h else unless(at_end("lon", False), lon_low[p])
    after = unless(at_end("lon", True), lon_high[p]) if h else x3[1][0]
    sums = advance(
        rows, (x3[h], 0), before, after,
        (x2, first), (cross, 0), (lev_low.at[p], first), (lev_high.at[p], first), (c3, first), (s3, first), (out, 0),
        None if faces is None else ((faces[2].at[p], first), (faces[3].at[p], first)), sums,
        jnp.logical_or(at_end("lat", False), at_end("lat", True)),
    )
    if faces is not None:
        if h:
            faces[1][p] = out[rows - 1]
        else:
            faces[0][p] = out[0]
    return sums


def edge_a(x2, x3a, x3b, cross, ll, lh, vl, vh, c3, s3, out, *faces):
    edge_half(0, x2, (x3a, x3b), cross, (ll, lh, vl, vh), c3, s3, out, faces)


def edge_b(x2, x3a, x3b, cross, ll, lh, vl, vh, c3, s3, a0, a1, a2, a3, out, *faces):
    edge_half(1, x2, (x3a, x3b), cross, (ll, lh, vl, vh), c3, s3, out, faces)


def edge_a_last(x2, x3a, x3b, cross, ll, lh, vl, vh, c3, s3, out, raw):
    raw[0], raw[1] = moments(out, edge_half(0, x2, (x3a, x3b), cross, (ll, lh, vl, vh), c3, s3, out, None, no_sums()))


def edge_b_last(x2, x3a, x3b, cross, ll, lh, vl, vh, c3, s3, raw, out, stats):
    mean, square = moments(out, edge_half(1, x2, (x3a, x3b), cross, (ll, lh, vl, vh), c3, s3, out, None, no_sums()))
    (_, a), (_, b) = CUTS
    stats[0, 0] = (a / NI) * raw[0] + (b / NI) * mean
    stats[1, 0] = raw[1] + square + (a * b / NI) * ((raw[0] - mean) * (raw[0] - mean))


def inner_first(
    tracer, c, s, x0, x2, x3a, x3b, on, ll, lh, vl, vh, a0, a1, a2, a3, q0, q1, q2, f0, f1, f2, f3, cc, ss, x1, sems
):
    loads = [[start(tracer.at[row_of(1)], x1, sems.at[6])], [], []]
    for p in (2, 1, 0):
        loads[p] += [start(c.at[row_of(p)], cc.at[p], sems.at[p]), start(s.at[row_of(p)], ss.at[p], sems.at[3 + p])]
    loads[2] += loads[0][:1]
    loads[0] = loads[0][1:]

    def ready(p):
        for copy in loads[p]:
            copy.wait()

    inner_planes(
        (x0, x1, x2, x3a, x3b), on, (ll, lh, vl, vh), [(cc.at[p], ss.at[p]) for p in range(3)], (q0, q1, q2),
        (f0, f1, f2, f3), ready=ready,
    )


def inner(x0, x1, x2, x3a, x3b, on, ll, lh, vl, vh, cc, ss, a0, a1, a2, a3, q0, q1, q2, *faces):
    inner_planes(
        (x0, x1, x2, x3a, x3b), on, (ll, lh, vl, vh), [(cc.at[p], ss.at[p]) for p in range(3)], (q0, q1, q2), faces
    )


def inner_last(x0, x1, x2, x3a, x3b, on, ll, lh, vl, vh, cc, ss, q0, q1, q2, stats, end, sems):
    outs, copies = ((q0, q1, q2), [])

    def done(p, h):
        rows = pl.ds(*CUTS[h])
        copies.append(start(outs[p].at[rows], end.at[row_of(p), rows], sems.at[2 * p + h]))

    inner_planes(
        (x0, x1, x2, x3a, x3b), on, (ll, lh, vl, vh), [(cc.at[p], ss.at[p]) for p in range(3)], outs, None, stats,
        done=done,
    )
    for copy in copies:
        copy.wait()


def scaled(parts, p, stats):
    means = [part[0, p] for part in stats]
    mean = sum(means[1:], means[0]) * (1.0 / parts)
    square = sum([part[1, p] for part in stats[1:]], stats[0][1, p])
    for m in means:
        square = square + NI * ((m - mean) * (m - mean))
    return mean, lax.rsqrt(square * (1.0 / (parts * NI)) + 0.0001)


def scale_rows(q, mean, scale, out):
    def block(b, _):
        i0 = b * UNROLL
        for r in range(UNROLL):
            out[i0 + r] = (q[i0 + r] - mean) * scale
        return 0

    lax.fori_loop(0, q.shape[0] // UNROLL, block, 0)


def scale_inner(parts):
    def kernel(q0, q1, q2, q3a, q3b, *rest):
        stats, (_, out, end, buffers, sems) = rest[:parts], rest[parts:]
        copies = [start(q, end.at[row_of(3), pl.ds(*CUTS[h])], sems.at[3 + h]) for h, q in enumerate((q3a, q3b))]
        for p, q in enumerate((q0, q1, q2)):
            scale_rows(q, *scaled(parts, p, stats), buffers.at[p])
            copies.append(start(buffers.at[p], out.at[row_of(p)], sems.at[p]))
        for copy in copies:
            copy.wait()

    return kernel


def scale_edge(parts):
    def kernel(q3a, q3b, *rest):
        stats, (_, out, buffer, sems) = rest[:parts], rest[parts:]
        mean, scale = scaled(parts, 0, stats)
        copies = []
        for h, q in enumerate((q3a, q3b)):
            for first in range(0, CUTS[h][1], PIECE):
                rows = pl.ds(CUTS[h][0] + first, PIECE)
                scale_rows(q.at[pl.ds(first, PIECE)], mean, scale, buffer.at[rows])
                copies.append(start(buffer.at[rows], out.at[row_of(3), rows], sems.at[len(copies)]))
        for copy in copies:
            copy.wait()

    return kernel


def turns(n):
    return range(n - 1, 0, -1)


def shards(tracer, c, s):
    lats, lons = (lax.axis_size(a) for a in ("lat", "lon"))
    on_pairs = [(i, i ^ 1) for i in range(lats)]
    cross_pairs = [(i, (((i + 1) ^ 1) - 1) % lats) for i in range(lats)]
    inside_pairs = cross_pairs[1:-1]

    def rotated(array, axis, by):
        n = lax.axis_size(axis)
        return lax.ppermute(array, axis, [(i, (i + by) % n) for i in range(n)])

    def of_everyone(array):
        return [array] + [rotated(array, "lon", by) for by in turns(lons)]

    def exchanged(faces):
        lon_low, lon_high, lev_low, lev_high = faces
        lev = (rotated(lev_high, "lev", 1), rotated(lev_low, "lev", -1))
        return [rotated(lon_high, "lon", 1), rotated(lon_low, "lon", -1), *lev]

    def swapped(q, pairs):
        return lax.ppermute(q, "lat", pairs)

    vm = lambda *arrays: [(a, VMEM) for a in arrays]
    dma = pltpu.SemaphoreType.DMA
    half, plane, face_outs = ([(shape, VMEM) for shape in PARTS], (PLANE, VMEM), [(f, VMEM) for f in FACES])
    inner_fields = ((3, *PLANE), VMEM)

    (x3a,) = call(first, [(tracer, HBM)], [half[0]], scratch=[dma((4,))])
    x3b, x0, *faces = call(messages, [(tracer, HBM)], [half[1], plane] + face_outs, scratch=[dma((2 + 4 * NJ,))])
    cross = [swapped(x3a, cross_pairs), swapped(x3b, cross_pairs)]
    on = swapped(x0, on_pairs)
    halo = exchanged(faces)
    x2, c3, s3 = call(load_edge, [(a, HBM) for a in (tracer, c, s)], [plane] * 3, scratch=[dma((3,))])

    for step in range(STEPS):
        edge = vm(x2, x3a, x3b)
        rest = vm(*halo, c3, s3)
        if step < STEPS - 1:
            qa, *faces = call(edge_a, edge + vm(cross[0]) + rest, [half[0]] + face_outs)
            cross[0] = swapped(qa, cross_pairs)
            outs = [plane] * 3 + face_outs
            if step == 0:
                q0, q1, q2, *faces, cc, ss = call(
                    inner_first,
                    [(a, HBM) for a in (tracer, c, s)] + vm(x0, x2, x3a, x3b, on, *halo, *faces),
                    outs + [inner_fields] * 2, scratch=[pltpu.VMEM(PLANE, F32), dma((7,))],
                    aliases={12 + n: 3 + n for n in range(4)}, limit=6 << 20,
                )
            else:
                q0, q1, q2, *faces = call(
                    inner, vm(x0, x1, x2, x3a, x3b, on, *halo, cc, ss, *faces), outs,
                    aliases={12 + n: 3 + n for n in range(4)},
                )
            on = swapped(q0, on_pairs)
            qb, *faces = call(
                edge_b, edge + vm(cross[1]) + rest + vm(*faces), [half[1]] + face_outs,
                aliases={10 + n: 1 + n for n in range(4)},
            )
            cross[1] = swapped(qb, inside_pairs)
            halo = exchanged(faces)
        else:
            q0, q1, q2, stats, end = call(
                inner_last, vm(x0, x1, x2, x3a, x3b, on, *halo, cc, ss),
                [plane] * 3 + [((2, 3, NK, NM), VMEM), ((NJ, *PLANE), HBM)], scratch=[dma((6,))],
            )
            inner_stats = of_everyone(stats)
            qa, raw = call(edge_a_last, edge + vm(cross[0]) + rest, [half[0], ((2, NK, NM), VMEM)])
            qb, stats = call(edge_b_last, edge + vm(cross[1]) + rest + vm(raw), [half[1], ((2, 1, NK, NM), VMEM)])
            edge_stats = of_everyone(stats)
        x0, x1, x2, x3a, x3b = q0, q1, q2, qa, qb

    out, end = call(
        scale_inner(lons), vm(x0, x1, x2, x3a, x3b, *inner_stats) + [(end, HBM)],
        [((NJ, *PLANE), HBM)] * 2, scratch=[pltpu.VMEM((3, *PLANE), F32), dma((5,))],
        aliases={5 + lons: 1}, limit=10 << 20,
    )
    (out,) = call(
        scale_edge(lons), vm(x3a, x3b, *edge_stats) + [(out, HBM)], [((NJ, *PLANE), HBM)],
        scratch=[pltpu.VMEM(PLANE, F32), dma((NI // PIECE,))], aliases={2 + lons: 0}, limit=6 << 20,
    )
    return out, end


def solution(mesh):
    placed = P("lat", "lon", "lev", None)

    return jax.shard_map(
        shards, mesh=mesh, in_specs=(placed, placed, placed), out_specs=(placed, placed), check_vma=False
    )
```
